32 devices in a mesh: dp: 16 (over z, y, x), tensor: 2 (over core).
Axes of the slice: x: 2, y: 2, z: 4, core: 2. Of those that a mesh axis runs over, the one named last changes fastest.
Arguments:
- inputs: bfloat16 [2, 16, 512, 768], P(None, 'dp', 'tensor'), may hold values from -6 to 6
- w_qkv: bfloat16 [3, 768, 768], P(None, 'dp', 'tensor'), may hold values from -0.21875 to 0.21875
- qv_bias: bfloat16 [2, 768], P(None, 'tensor'), may hold values from -3 to 3
- w_out: bfloat16 [768, 768], P('tensor', 'dp'), may hold values from -2.5 to 2.5
- out_bias: bfloat16 [768], replicated, may hold values from -3 to 3
- norm1_gain: bfloat16 [768], replicated, may hold values from 0.099609375 to 1.8984375
- norm1_shift: bfloat16 [768], replicated, may hold values from -3 to 3
- w_in: bfloat16 [768, 3072], P('dp', 'tensor'), may hold values from -0.21875 to 0.21875
- ffn_bias: bfloat16 [3072], P('tensor'), may hold values from -3 to 3
- w_down: bfloat16 [3072, 768], P('tensor', 'dp'), may hold values from -0.109375 to 0.109375
- down_bias: bfloat16 [768], replicated, may hold values from -3 to 3
- norm2_gain: bfloat16 [768], replicated, may hold values from 0.099609375 to 1.8984375
- norm2_shift: bfloat16 [768], replicated, may hold values from -3 to 3
- attn_drop: int32 [2, 16, 512, 768], P(None, 'dp', 'tensor'), may hold values 0 or 1
- ffn_drop: int32 [2, 16, 512, 768], P(None, 'dp', 'tensor'), may hold values 0 or 1
- lengths: int32 [16], P('dp'), may hold values from 128 to 512, as said below
- cotangent: bfloat16 [2, 16, 512, 768], P(None, 'dp', 'tensor'), may hold values from -6 to 6
- pooled: float32 [2, 16, 768], P(None, 'dp'), may hold values from -50 to 50
- positive: int32 [16], P('dp'), may hold values from 0 to 15, each once
Outputs:
- output: bfloat16 [2, 16, 512, 768], P(None, 'dp', 'tensor')
- input_grad: bfloat16 [2, 16, 512, 768], P(None, 'dp', 'tensor')
- grad_w_qkv: float32 [3, 768, 768], P(None, 'dp', 'tensor')
- grad_qv_bias: float32 [2, 768], P(None, 'tensor')
- grad_w_out: float32 [768, 768], P('tensor', 'dp')
- grad_out_bias: float32 [768], replicated
- grad_norm1_gain: float32 [768], replicated
- grad_norm1_shift: float32 [768], replicated
- grad_w_in: float32 [768, 3072], P('dp', 'tensor')
- grad_ffn_bias: float32 [3072], P('tensor')
- grad_w_down: float32 [3072, 768], P('tensor', 'dp')
- grad_down_bias: float32 [768], replicated
- grad_norm2_gain: float32 [768], replicated
- grad_norm2_shift: float32 [768], replicated
- loss: float32 [], replicated
The draws below stay inside these ranges and needn't reach their ends.
Inputs may be any that keep to these rules, and one draw needn't show every extreme that they name: `lengths`: the length is the same in both views; positions from it on are padding; some sentence has exactly 512.
All inputs are finite; a program needn't handle non-finite values. No bound on the sum of `attn_drop` or of `ffn_drop` on one device may be relied on, other than what follows from the above.
Results may differ from the reference program's by a relative error of at most 0.02.
Values may be sent and summed in bfloat16 or wider, within the bound.
A program may use at most 192 MiB of HBM per device.

```python
import math
import jax
import jax.numpy as jnp
from jax import lax

D = 768
HEADS = 12
HEAD_DIM = 64
FF = 3072
SEQ = 512
VIEWS = 2
SENTS = 16


def draw_lengths(key, part):
    spread = jax.random.randint(jax.random.fold_in(key, 11), (SENTS,), SEQ // 4, SEQ + 1)
    longest = jax.random.randint(jax.random.fold_in(key, 12), (), 0, SENTS)
    return jnp.where(jnp.arange(SENTS) == longest, SEQ, spread).astype(jnp.int32)


def draw_pooled(key, part):
    levels = jnp.exp(jax.random.uniform(jax.random.fold_in(key, 21), (D,), jnp.float32) * math.log(10.0))
    base = jnp.clip(jax.random.normal(jax.random.fold_in(key, 22), (2, SENTS, D), jnp.float32), -5.0, 5.0)
    return (base * levels[None, None, :]).astype(jnp.float32)


def touch_ends(values, own_key, smallest, high):
    place = [jax.random.randint(jax.random.fold_in(own_key, axis), (), 0, length) for axis, length in enumerate(values.shape)]
    widest = values.shape.index(max(values.shape))
    next_to = place[:widest] + [(place[widest] + 1) % values.shape[widest]] + place[widest + 1:]
    return values.at[tuple(place)].set(smallest).at[tuple(next_to)].set(high)


def shard_levels(rng, shape, pieces, least, largest):
    level, own = 1.0, jax.random.fold_in(rng, 6)
    for axis_at, parts in pieces:
        heights = jnp.exp(jax.random.uniform(jax.random.fold_in(own, axis_at), (parts,), jnp.float32, least / len(pieces), largest / len(pieces)))
        level = level * jnp.repeat(heights, shape[axis_at] // parts).reshape([-1 if axis == axis_at else 1 for axis in range(len(shape))])
    return level


def bell_draw(key, extent, deviation, reach, split=(), held_as=jnp.bfloat16):
    entries = deviation * jax.random.normal(key, extent, jnp.float32)
    if split:
        entries = entries * shard_levels(key, extent, split, -0.22, 0.18)
    return jnp.clip(entries, -reach, reach).astype(held_as)


def setup_inputs(seed: int = 0) -> dict:
    key_list = jax.random.split(jax.random.key(seed), 20)
    return {
        "inputs": bell_draw(key_list[0], (VIEWS, SENTS, SEQ, D), 1.0, 6.0, ((1, 16), (2, 2))),
        "w_qkv": bell_draw(key_list[1], (3, D, D), D ** -0.5, 0.21875, ((1, 16), (2, 2))),
        "qv_bias": bell_draw(key_list[2], (2, D), 0.5, 3.0, ((1, 2),)),
        "w_out": bell_draw(key_list[3], (D, D), (max(D // 128, 1)) ** -0.5, 2.5, ((0, 2), (1, 16))),
        "out_bias": bell_draw(key_list[4], (D,), 0.5, 3.0),
        "norm1_gain": jnp.clip(1.0 + 0.18 * jax.random.normal(key_list[5], (D,), jnp.float32), 0.099609375, 1.8984375).astype(jnp.bfloat16),
        "norm1_shift": bell_draw(key_list[6], (D,), 0.5, 3.0),
        "w_in": bell_draw(key_list[7], (D, FF), D ** -0.5, 0.21875, ((0, 16), (1, 2))),
        "ffn_bias": bell_draw(key_list[8], (FF,), 0.5, 3.0, ((0, 2),)),
        "w_down": bell_draw(key_list[9], (FF, D), FF ** -0.5, 0.109375, ((0, 2), (1, 16))),
        "down_bias": bell_draw(key_list[10], (D,), 0.5, 3.0),
        "norm2_gain": jnp.clip(1.0 + 0.18 * jax.random.normal(key_list[11], (D,), jnp.float32), 0.099609375, 1.8984375).astype(jnp.bfloat16),
        "norm2_shift": bell_draw(key_list[12], (D,), 0.5, 3.0),
        "attn_drop": touch_ends((jax.random.randint(key_list[13], (VIEWS, SENTS, SEQ, D), 0, 10) < 9).astype(jnp.int32), jax.random.fold_in(key_list[13], 1), 0, 1),
        "ffn_drop": touch_ends((jax.random.randint(key_list[14], (VIEWS, SENTS, SEQ, D), 0, 10) < 9).astype(jnp.int32), jax.random.fold_in(key_list[14], 1), 0, 1),
        "lengths": draw_lengths(jax.random.fold_in(key_list[19], 71), 0),
        "cotangent": bell_draw(key_list[16], (VIEWS, SENTS, SEQ, D), 1.0, 6.0, ((1, 16), (2, 2))),
        "pooled": draw_pooled(jax.random.fold_in(key_list[19], 71), 0),
        "positive": jax.random.permutation(key_list[18], SENTS).astype(jnp.int32),
    }


KEEP_RATE = 0.9
NORM_EPS = 1e-05
TEMPER = 0.05
HIGH = lax.Precision.HIGHEST

@jax.custom_vjp
def low(v):
    return lax.optimization_barrier(v.astype(jnp.bfloat16)).astype(jnp.float32)

@jax.custom_vjp
def low_back(v):
    return v

def low_keep(v):
    return (low(v), None)

def low_pass(kept, grad):
    return (grad,)

def back_keep(v):
    return (v, None)

def back_low(kept, grad):
    return (low(grad),)
low.defvjp(low_keep, low_pass)
low_back.defvjp(back_keep, back_low)

def both_ways(v):
    return low(low_back(v))

def gelu_value(u):
    return 0.5 * u * (1.0 + jax.scipy.special.erf(u * 0.7071067811865476))

def normalize(rows, gain, shift):
    centre = rows - lax.optimization_barrier(jnp.mean(rows, axis=-1, keepdims=True))
    scale = lax.rsqrt(lax.optimization_barrier(jnp.mean(centre * centre, axis=-1, keepdims=True)) + NORM_EPS)
    return centre * scale * gain + shift

def split_heads(matrix):
    return matrix.reshape(SEQ, HEADS, HEAD_DIM)

def layer(x, params, drop_one, drop_two, length):
    w_qkv, qv_bias, w_out, out_bias, gain_one, shift_one, w_in, ffn_bias, w_down, down_bias, gain_two, shift_two = params
    rows = low_back(x)
    query = both_ways(jnp.dot(rows, w_qkv[0], precision=HIGH) + qv_bias[0])
    keys = both_ways(jnp.dot(rows, w_qkv[1], precision=HIGH))
    values = both_ways(jnp.dot(rows, w_qkv[2], precision=HIGH) + qv_bias[1])
    scores = low_back(jnp.einsum('qhd,khd->hqk', split_heads(query), split_heads(keys), precision=HIGH) * 0.125)
    valid = jnp.arange(SEQ) < length
    scores = jnp.where(valid[None, None, :], scores, -1e+30)
    probs = jax.nn.softmax(scores, axis=-1)
    mixed = jnp.einsum('hqk,khd->qhd', low(probs), split_heads(values), precision=HIGH).reshape(SEQ, D)
    mixed = both_ways(mixed)
    branch = low_back(jnp.dot(mixed, w_out, precision=HIGH) + out_bias)
    first = normalize(rows + drop_one * branch / KEEP_RATE, gain_one, shift_one)
    hidden = low_back(jnp.dot(low(first), w_in, precision=HIGH) + ffn_bias)
    acted = low(gelu_value(hidden))
    second = low_back(jnp.dot(acted, w_down, precision=HIGH) + down_bias)
    return normalize(first + drop_two * second / KEEP_RATE, gain_two, shift_two)

def reference(inputs, w_qkv, qv_bias, w_out, out_bias, norm1_gain, norm1_shift, w_in, ffn_bias, w_down, down_bias, norm2_gain, norm2_shift, attn_drop, ffn_drop, lengths, cotangent, pooled, positive):
    params = tuple((p.astype(jnp.float32) for p in (w_qkv, qv_bias, w_out, out_bias, norm1_gain, norm1_shift, w_in, ffn_bias, w_down, down_bias, norm2_gain, norm2_shift)))
    count = VIEWS * SENTS
    rows_all = inputs.reshape(count, SEQ, D)
    drops_one = attn_drop.reshape(count, SEQ, D)
    drops_two = ffn_drop.reshape(count, SEQ, D)
    grads_out = cotangent.reshape(count, SEQ, D)
    lens = jnp.tile(lengths, VIEWS)

    def step(total, item):
        rows, first_mask, second_mask, length, grad_out = item

        def forward(xv, pv):
            return layer(xv, pv, first_mask.astype(jnp.float32), second_mask.astype(jnp.float32), length)
        result, pull = jax.vjp(forward, rows.astype(jnp.float32), params)
        grad_rows, grad_params = pull(grad_out.astype(jnp.float32))
        total = jax.tree.map(lambda a, b: a + b, total, grad_params)
        return (total, (result.astype(jnp.bfloat16), grad_rows.astype(jnp.bfloat16)))
    zeros = jax.tree.map(jnp.zeros_like, params)
    totals, (results, grad_rows) = lax.scan(step, zeros, (rows_all, drops_one, drops_two, lens, grads_out))
    output = results.reshape(VIEWS, SENTS, SEQ, D)
    input_grad = grad_rows.reshape(VIEWS, SENTS, SEQ, D)
    anchor = pooled[0]
    other = pooled[1]
    anchor = anchor * lax.rsqrt(lax.optimization_barrier(jnp.sum(anchor * anchor, axis=-1, keepdims=True)) + 1e-06)
    other = other * lax.rsqrt(lax.optimization_barrier(jnp.sum(other * other, axis=-1, keepdims=True)) + 1e-06)
    logits = jnp.dot(anchor, other.T, precision=HIGH) / TEMPER
    top = lax.optimization_barrier(jnp.max(logits, axis=-1, keepdims=True))
    spread = top[:, 0] + jnp.log(lax.optimization_barrier(jnp.sum(jnp.exp(logits - top), axis=-1)))
    picked = jnp.take_along_axis(logits, positive[:, None].astype(jnp.int32), axis=1)[:, 0]
    loss = jnp.mean(spread - picked)
    return (output, input_grad, totals[0], totals[1], totals[2], totals[3], totals[4], totals[5], totals[6], totals[7], totals[8], totals[9], totals[10], totals[11], loss)
```

```python
import functools

import jax
import jax.numpy as jnp
from jax import lax
from jax.experimental import pallas as pl
from jax.experimental.pallas import tpu as pltpu
from jax.sharding import PartitionSpec as P

HEAD_DIM = 64


KEEP_RATE = 0.9
NORM_EPS = 1e-05
TEMPER = 0.05
HIGH = lax.Precision.HIGHEST


def gelu_value(u):
    return 0.5 * u * (1.0 + jax.scipy.special.erf(u * 0.7071067811865476))


def gelu_slope(u):
    return (
        0.5 * (1.0 + jax.scipy.special.erf(u * 0.7071067811865476))
        + u * jnp.exp(-0.5 * u * u) * 0.3989422804014327
    )


def normalize(rows, gain, shift):
    centre = rows - jnp.mean(rows, axis=-1, keepdims=True)
    scale = lax.rsqrt(jnp.mean(centre * centre, axis=-1, keepdims=True) + NORM_EPS)
    unit = centre * scale
    return (unit * gain + shift, unit, scale)


def normalize_back(grad, unit, scale, gain):
    inner = grad * gain
    return scale * (
        inner
        - jnp.mean(inner, axis=-1, keepdims=True)
        - unit * jnp.mean(inner * unit, axis=-1, keepdims=True)
    )


def column_sum(values):
    return jnp.sum(values.astype(jnp.float32), axis=tuple(range(values.ndim - 1)))


def gather_weights(w_qkv, w_out, w_in, w_down):
    return (
        lax.all_gather(w_qkv, "dp", axis=1, tiled=True),
        lax.all_gather(w_out, "dp", axis=1, tiled=True),
        lax.all_gather(w_in, "dp", axis=0, tiled=True),
        lax.all_gather(w_down, "dp", axis=1, tiled=True),
    )


def attend(query, keys, values, key_ok, block):
    sents, seq, heads, width = query.shape
    count = seq // block
    q_blocks = jnp.moveaxis(query.reshape(sents, count, block, heads, width), 1, 0)

    def one_block(q_block):
        scores = (
            jnp.einsum("bqhd,bkhd->bhqk", q_block, keys, preferred_element_type=jnp.float32) * 0.125
        )
        scores = jnp.where(key_ok[:, None, None, :], scores, -1e30)
        top = jnp.max(scores, axis=-1, keepdims=True)
        raised = jnp.exp(scores - top)
        total = jnp.sum(raised, axis=-1, keepdims=True)
        probs = (raised / total).astype(jnp.bfloat16)
        mixed = jnp.einsum("bhqk,bkhd->bqhd", probs, values, preferred_element_type=jnp.float32)
        return (mixed, top[..., 0] + jnp.log(total[..., 0]))

    mixed, spread = lax.map(one_block, q_blocks)
    mixed = jnp.moveaxis(mixed, 0, 1).reshape(sents, seq, heads * width)
    return (mixed, spread)


def attend_back(query, keys, values, key_ok, spread, grad_mixed, block):
    sents, seq, heads, width = query.shape
    count = seq // block
    q_blocks = jnp.moveaxis(query.reshape(sents, count, block, heads, width), 1, 0)
    g_blocks = jnp.moveaxis(grad_mixed.reshape(sents, count, block, heads, width), 1, 0)

    def one_block(carry, item):
        grad_keys, grad_values = carry
        q_block, g_block, s_block = item
        scores = (
            jnp.einsum("bqhd,bkhd->bhqk", q_block, keys, preferred_element_type=jnp.float32) * 0.125
        )
        scores = jnp.where(key_ok[:, None, None, :], scores, -1e30)
        probs = jnp.exp(scores - s_block[..., None])
        grad_probs = jnp.einsum(
            "bqhd,bkhd->bhqk", g_block, values, preferred_element_type=jnp.float32
        )
        grad_scores = (
            probs * (grad_probs - jnp.sum(probs * grad_probs, axis=-1, keepdims=True))
        ).astype(jnp.bfloat16)
        grad_query = (
            jnp.einsum("bhqk,bkhd->bqhd", grad_scores, keys, preferred_element_type=jnp.float32)
            * 0.125
        )
        grad_keys = (
            grad_keys
            + jnp.einsum(
                "bhqk,bqhd->bkhd", grad_scores, q_block, preferred_element_type=jnp.float32
            )
            * 0.125
        )
        grad_values = grad_values + jnp.einsum(
            "bhqk,bqhd->bkhd",
            probs.astype(jnp.bfloat16),
            g_block,
            preferred_element_type=jnp.float32,
        )
        return ((grad_keys, grad_values), grad_query)

    zero = jnp.zeros((sents, seq, heads, width), jnp.float32)
    (grad_keys, grad_values), grad_query = lax.scan(
        one_block, (zero, zero), (q_blocks, g_blocks, spread)
    )
    grad_query = jnp.moveaxis(grad_query, 0, 1).reshape(sents, seq, heads * width)
    return (
        grad_query,
        grad_keys.reshape(sents, seq, heads * width),
        grad_values.reshape(sents, seq, heads * width),
    )


def shards(
    inputs,
    w_qkv,
    qv_bias,
    w_out,
    out_bias,
    norm1_gain,
    norm1_shift,
    w_in,
    ffn_bias,
    w_down,
    down_bias,
    norm2_gain,
    norm2_shift,
    attn_drop,
    ffn_drop,
    lengths,
    cotangent,
    pooled,
    positive,
):
    views, sents, local_seq, width = inputs.shape
    seq = local_seq * lax.axis_size("tensor")
    block = min(512, seq)
    heads = w_qkv.shape[2] // HEAD_DIM
    key_ok = jnp.arange(seq)[None, :] < lengths[:, None]
    gain_one = norm1_gain.astype(jnp.float32)
    shift_one = norm1_shift.astype(jnp.float32)
    gain_two = norm2_gain.astype(jnp.float32)
    shift_two = norm2_shift.astype(jnp.float32)
    bias_out = out_bias.astype(jnp.float32)
    bias_down = down_bias.astype(jnp.float32)
    bias_ffn = ffn_bias.astype(jnp.float32)
    bias_qkv = jnp.stack([qv_bias[0], jnp.zeros_like(qv_bias[0]), qv_bias[1]]).astype(jnp.float32)
    shard_grads = tuple((jnp.zeros(w.shape, jnp.float32) for w in (w_qkv, w_out, w_in, w_down)))
    acc_gain_one = jnp.zeros((width,), jnp.float32)
    acc_shift_one = jnp.zeros((width,), jnp.float32)
    acc_gain_two = jnp.zeros((width,), jnp.float32)
    acc_shift_two = jnp.zeros((width,), jnp.float32)
    acc_out_bias = jnp.zeros((width,), jnp.float32)
    acc_down_bias = jnp.zeros((width,), jnp.float32)
    acc_ffn_bias = jnp.zeros(ffn_bias.shape, jnp.float32)
    acc_qv_bias = jnp.zeros(qv_bias.shape, jnp.float32)
    outputs = []
    input_grads = []
    for view in range(views):
        whole = gather_weights(w_qkv, w_out, w_in, w_down)
        full_qkv, full_out, full_in, full_down = whole
        rows = inputs[view]
        full_rows = lax.all_gather(rows, "tensor", axis=1, tiled=True)
        qkv = jnp.einsum("bsd,cde->cbse", full_rows, full_qkv, preferred_element_type=jnp.float32)
        qkv = (qkv + bias_qkv[:, None, None, :]).astype(jnp.bfloat16)
        split = qkv.reshape(3, sents, seq, heads, HEAD_DIM)
        mixed, spread = attend(split[0], split[1], split[2], key_ok, block)
        mixed = mixed.astype(jnp.bfloat16)
        partial_branch = jnp.einsum(
            "bse,ed->bsd", mixed, full_out, preferred_element_type=jnp.float32
        )
        branch = (
            lax.psum_scatter(
                partial_branch.astype(jnp.bfloat16), "tensor", scatter_dimension=1, tiled=True
            ).astype(jnp.float32)
            + bias_out
        )
        drop_one = attn_drop[view].astype(jnp.float32) / KEEP_RATE
        first, unit_one, scale_one = normalize(
            rows.astype(jnp.float32) + drop_one * branch, gain_one, shift_one
        )
        full_first = lax.all_gather(first.astype(jnp.bfloat16), "tensor", axis=1, tiled=True)
        hidden = (
            jnp.einsum("bsd,df->bsf", full_first, full_in, preferred_element_type=jnp.float32)
            + bias_ffn
        )
        acted = gelu_value(hidden).astype(jnp.bfloat16)
        partial_second = jnp.einsum(
            "bsf,fd->bsd", acted, full_down, preferred_element_type=jnp.float32
        )
        second = (
            lax.psum_scatter(
                partial_second.astype(jnp.bfloat16), "tensor", scatter_dimension=1, tiled=True
            ).astype(jnp.float32)
            + bias_down
        )
        drop_two = ffn_drop[view].astype(jnp.float32) / KEEP_RATE
        result, unit_two, scale_two = normalize(first + drop_two * second, gain_two, shift_two)
        outputs.append(result.astype(jnp.bfloat16))
        full_qkv, full_out, full_in, full_down = gather_weights(w_qkv, w_out, w_in, w_down)
        grad_out = cotangent[view].astype(jnp.float32)
        acc_gain_two = acc_gain_two + column_sum(grad_out * unit_two)
        acc_shift_two = acc_shift_two + column_sum(grad_out)
        grad_two = normalize_back(grad_out, unit_two, scale_two, gain_two)
        grad_second = (grad_two * drop_two).astype(jnp.bfloat16)
        full_second = lax.all_gather(grad_second, "tensor", axis=1, tiled=True)
        grad_w_down = jnp.einsum(
            "bsf,bsd->fd", acted, full_second, preferred_element_type=jnp.float32
        )
        acc_down_bias = acc_down_bias + column_sum(full_second)
        grad_acted = jnp.einsum(
            "bsd,fd->bsf", full_second, full_down, preferred_element_type=jnp.float32
        )
        grad_hidden = (grad_acted * gelu_slope(hidden)).astype(jnp.bfloat16)
        grad_w_in = jnp.einsum(
            "bsd,bsf->df", full_first, grad_hidden, preferred_element_type=jnp.float32
        )
        acc_ffn_bias = acc_ffn_bias + column_sum(grad_hidden)
        partial_first = jnp.einsum(
            "bsf,df->bsd", grad_hidden, full_in, preferred_element_type=jnp.float32
        )
        grad_first = grad_two + lax.psum_scatter(
            partial_first.astype(jnp.bfloat16), "tensor", scatter_dimension=1, tiled=True
        ).astype(jnp.float32)
        acc_gain_one = acc_gain_one + column_sum(grad_first * unit_one)
        acc_shift_one = acc_shift_one + column_sum(grad_first)
        grad_one = normalize_back(grad_first, unit_one, scale_one, gain_one)
        grad_branch = (grad_one * drop_one).astype(jnp.bfloat16)
        full_branch = lax.all_gather(grad_branch, "tensor", axis=1, tiled=True)
        grad_w_out = jnp.einsum(
            "bse,bsd->ed", mixed, full_branch, preferred_element_type=jnp.float32
        )
        acc_out_bias = acc_out_bias + column_sum(full_branch)
        grad_mixed = jnp.einsum(
            "bsd,ed->bse", full_branch, full_out, preferred_element_type=jnp.float32
        ).astype(jnp.bfloat16)
        grad_query, grad_keys, grad_values = attend_back(
            split[0],
            split[1],
            split[2],
            key_ok,
            spread,
            grad_mixed.reshape(sents, seq, heads, HEAD_DIM),
            block,
        )
        grad_qkv = jnp.stack([grad_query, grad_keys, grad_values]).astype(jnp.bfloat16)
        grad_w_qkv = jnp.einsum(
            "bsd,cbse->cde", full_rows, grad_qkv, preferred_element_type=jnp.float32
        )
        acc_qv_bias = acc_qv_bias + jnp.stack([column_sum(grad_qkv[0]), column_sum(grad_qkv[2])])
        partial_rows = jnp.einsum(
            "cbse,cde->bsd", grad_qkv, full_qkv, preferred_element_type=jnp.float32
        )
        grad_rows = grad_one + lax.psum_scatter(
            partial_rows.astype(jnp.bfloat16), "tensor", scatter_dimension=1, tiled=True
        ).astype(jnp.float32)
        input_grads.append(grad_rows.astype(jnp.bfloat16))
        local_grads = (grad_w_qkv, grad_w_out, grad_w_in, grad_w_down)
        summed = (
            lax.psum_scatter(local_grads[0], "dp", scatter_dimension=1, tiled=True),
            lax.psum_scatter(local_grads[1], "dp", scatter_dimension=1, tiled=True),
            lax.psum_scatter(local_grads[2], "dp", scatter_dimension=0, tiled=True),
            lax.psum_scatter(local_grads[3], "dp", scatter_dimension=1, tiled=True),
        )
        shard_grads = tuple((a + b for a, b in zip(shard_grads, summed)))
    anchor = pooled[0]
    other = pooled[1]
    anchor = anchor * lax.rsqrt(jnp.sum(anchor * anchor, axis=-1, keepdims=True) + 1e-06)
    other = other * lax.rsqrt(jnp.sum(other * other, axis=-1, keepdims=True) + 1e-06)
    every = lax.all_gather(other, "dp", axis=0, tiled=True)
    logits = jnp.dot(anchor, every.T, precision=HIGH) / TEMPER
    top = jnp.max(logits, axis=-1, keepdims=True)
    log_total = top[:, 0] + jnp.log(jnp.sum(jnp.exp(logits - top), axis=-1))
    chosen = jnp.arange(every.shape[0])[None, :] == positive[:, None]
    picked = jnp.sum(jnp.where(chosen, logits, 0.0), axis=-1)
    loss_term = jnp.sum(log_total - picked)
    sum_qv, sum_out, sum_ffn, sum_down = lax.psum(
        (acc_qv_bias, acc_out_bias, acc_ffn_bias, acc_down_bias), "dp"
    )
    sum_gain_one, sum_shift_one, sum_gain_two, sum_shift_two, loss_sum = lax.psum(
        (acc_gain_one, acc_shift_one, acc_gain_two, acc_shift_two, loss_term), ("dp", "tensor")
    )
    loss = loss_sum / (every.shape[0] * lax.axis_size("tensor"))
    return (
        jnp.stack(outputs),
        jnp.stack(input_grads),
        shard_grads[0],
        sum_qv,
        shard_grads[1],
        sum_out,
        sum_gain_one,
        sum_shift_one,
        shard_grads[2],
        sum_ffn,
        shard_grads[3],
        sum_down,
        sum_gain_two,
        sum_shift_two,
        loss,
    )


MESH = pl.DeviceIdType.MESH
VMEM = pltpu.VMEM
DMA = pltpu.SemaphoreType.DMA
LINE = 4


def place():
    me = lax.axis_index("dp")
    core = lax.axis_index("tensor")
    z, q = me // 4, me % 4
    y, x = q // 2, q % 2
    over_y, over_x = (1 - y) * 2 + x, y * 2 + 1 - x
    near = (1 - core) * over_y + core * over_x
    far = core * over_y + (1 - core) * over_x
    return z, q, core, near, far, 3 - q


def greet(z, q, core):
    barrier = pltpu.get_barrier_semaphore()
    peers = [((z + k) % LINE * 4 + q, core) for k in (1, 2, 3)]
    y, x = q // 2, q % 2
    peers += [(z * 4 + (1 - y) * 2 + x, core), (z * 4 + y * 2 + 1 - x, core), (z * 4 + q, 1 - core)]
    for peer in peers:
        pl.semaphore_signal(barrier, inc=1, device_id=peer, device_id_type=MESH)
    pl.semaphore_wait(barrier, len(peers))


def remote(src, dst, send, recv, device):
    return pltpu.make_async_remote_copy(
        src_ref=src, dst_ref=dst, send_sem=send, recv_sem=recv, device_id=device, device_id_type=MESH
    )


class Gather:
    def __init__(self, shard, whole, send, recv, local, at, where):
        self.shard, self.whole, self.send, self.recv, self.local, self.at = shard, whole, send, recv, local, at
        self.where = where

    def part(self, z, q):
        return self.whole.at[self.at + (z, q)]

    def line(self, q):
        return self.whole.at[self.at + (slice(None), q)]

    def start(self):
        z, q, core, near, far, corner = self.where
        self.own = pltpu.make_async_copy(self.shard, self.part(z, q), self.local)
        self.own.start()
        self.along = []
        for k in (1, 3, 2):
            copy = remote(
                self.shard, self.part(z, q), self.send.at[k - 1], self.recv.at[k - 1], ((z + k) % LINE * 4 + q, core)
            )
            copy.start()
            self.along.append(copy)

    def spread(self):
        z, q, core, near, far, corner = self.where
        for copy in self.along:
            copy.wait_recv()
        self.own.wait()
        self.to_near = remote(self.line(q), self.line(q), self.send.at[3], self.recv.at[3], (z * 4 + near, core))
        self.to_far = remote(self.line(q), self.line(q), self.send.at[4], self.recv.at[4], (z * 4 + far, core))
        self.to_near.start()
        self.to_far.start()

    def forward(self):
        z, q, core, near, far, corner = self.where
        self.to_near.wait_recv()
        self.pass_on = remote(self.line(near), self.line(near), self.send.at[5], self.recv.at[5], (z * 4 + far, core))
        self.pass_on.start()

    def ready(self):
        self.to_far.wait_recv()
        self.pass_on.wait_recv()

    def finish(self):
        for copy in self.along + [self.to_near, self.to_far, self.pass_on]:
            copy.wait_send()


class Scatter:
    def __init__(self, grad, got_far, got_near, got_line, total, send, recv, where):
        self.grad, self.got_far, self.got_near, self.got_line = grad, got_far, got_near, got_line
        self.total, self.send, self.recv, self.where = total, send, recv, where

    def start(self):
        z, q, core, near, far, corner = self.where
        there = (z * 4 + far, core)
        self.far_own = remote(self.grad.at[:, far], self.got_far.at[0], self.send.at[0], self.recv.at[0], there)
        self.far_near = remote(self.grad.at[:, corner], self.got_far.at[1], self.send.at[1], self.recv.at[1], there)
        self.far_near.start()
        self.far_own.start()

    def second(self):
        z, q, core, near, far, corner = self.where
        self.far_near.wait_recv()

        def add(i, carry):
            self.grad[i, near] = (
                self.grad[i, near].astype(jnp.float32) + self.got_far[1, i].astype(jnp.float32)
            ).astype(jnp.bfloat16)
            return carry

        lax.fori_loop(0, LINE, add, 0)
        self.to_near = remote(
            self.grad.at[:, near], self.got_near, self.send.at[2], self.recv.at[2], (z * 4 + near, core)
        )
        self.to_near.start()

    def third(self):
        z, q, core, near, far, corner = self.where
        self.far_own.wait_recv()
        self.to_near.wait_recv()

        def sum_of(i):
            return (
                self.grad[i, q].astype(jnp.float32)
                + self.got_far[0, i].astype(jnp.float32)
                + self.got_near[i].astype(jnp.float32)
            )

        self.total[...] = sum_of(z)

        def add(i, carry):
            self.grad[i, q] = sum_of(i).astype(jnp.bfloat16)
            return carry

        lax.fori_loop(0, LINE, add, 0)
        self.along = []
        for k in (1, 3, 2):
            there = (z + k) % LINE
            copy = remote(
                self.grad.at[there, q], self.got_line.at[k - 1], self.send.at[2 + k], self.recv.at[2 + k],
                (there * 4 + q, core),
            )
            copy.start()
            self.along.append(copy)

    def last(self):
        for copy in self.along:
            copy.wait_recv()
        total = self.total[...]
        for k in range(3):
            total = total + self.got_line[k].astype(jnp.float32)
        self.total[...] = total

    def finish(self):
        for copy in self.along + [self.far_own, self.far_near, self.to_near]:
            copy.wait_send()


class Sum:
    def __init__(self, held, got, lines, send, recv, where):
        self.held, self.got, self.lines, self.send, self.recv, self.where = held, got, lines, send, recv, where

    def hop(self, n, device, rows):
        copy = remote(
            self.held.at[n, pl.ds(0, rows)], self.got.at[n, pl.ds(0, rows)], self.send.at[n], self.recv.at[n], device
        )
        copy.start()
        self.copy = copy

    def start(self):
        z, q, core, near, far, corner = self.where
        self.copies = []
        self.hop(0, (z * 4 + q, 1 - core), 8)

    def step(self, n):
        z, q, core, near, far, corner = self.where
        y, x = q // 2, q % 2
        self.copy.wait_recv()
        self.copies.append(self.copy)
        rows = self.held.shape[1]
        if n == 0:
            self.held[1, :8] = self.held[0, :8] + self.got[0, :8]
            self.held[1, 8:] = self.held[0, 8:]
            self.hop(1, (z * 4 + y * 2 + 1 - x, core), rows)
        elif n == 1:
            self.held[2] = self.held[1] + self.got[1]
            self.hop(2, (z * 4 + (1 - y) * 2 + x, core), rows)
        else:
            total = self.held[2] + self.got[2]
            self.held[3] = total
            self.lines[z] = total
            for k in (1, 2, 3):
                there = (z + k) % LINE
                copy = remote(
                    self.held.at[3], self.lines.at[z], self.send.at[2 + k], self.recv.at[2 + k], (there * 4 + q, core)
                )
                copy.start()
                self.copies.append(copy)

    def total(self):
        for copy in self.copies[3:]:
            copy.wait_recv()
        return (self.lines[0] + self.lines[1]) + (self.lines[2] + self.lines[3])

    def finish(self):
        for copy in self.copies:
            copy.wait_send()


def gather_kernel(qkv, out, w_in, down, pool, all_qkv, all_out, all_in, all_down, all_pool, send, recv, local):
    where = place()
    greet(*where[:3])
    pairs = [(qkv.at[i], all_qkv, (i,)) for i in range(3)]
    pairs += [(out, all_out, ()), (pool, all_pool, ()), (w_in, all_in, ()), (down, all_down, ())]
    groups = [
        Gather(shard, whole, send.at[n], recv.at[n], local.at[n], at, where) for n, (shard, whole, at) in enumerate(pairs)
    ]
    for group in groups:
        group.start()
    count = len(groups)
    for n in range(count + 1):
        if n < count:
            groups[n].spread()
        if n >= 1:
            groups[n - 1].forward()
    for group in groups:
        group.ready()
    for group in groups:
        group.finish()


def gather_all(qkv, out, w_in, down, pool):
    shapes = [(3, LINE, 4) + qkv.shape[1:]] + [(LINE, 4) + a.shape for a in (out, w_in, down, pool)]
    kinds = [jnp.bfloat16] * 4 + [jnp.float32]
    vmem = pl.BlockSpec(memory_space=pltpu.VMEM)
    return pl.pallas_call(
        gather_kernel,
        out_shape=[jax.ShapeDtypeStruct(s, d) for s, d in zip(shapes, kinds)],
        in_specs=[vmem] * 5,
        out_specs=[vmem] * 5,
        scratch_shapes=[DMA((7, 6)), DMA((7, 6)), DMA((7,))],
        compiler_params=pltpu.CompilerParams(collective_id=0, has_side_effects=True, vmem_limit_bytes=40 << 20),
        name="gather_weights",
    )(qkv, out, w_in, down, pool)


def scatter_kernel(count, *refs):
    grads, small, refs = refs[:count], refs[count], refs[count + 1 :]
    totals, summed, refs = refs[:count], refs[count], refs[count + 1 :]
    far, near, line = refs[:count], refs[count : 2 * count], refs[2 * count : 3 * count]
    held, got, lines, send, recv, small_send, small_recv = refs[3 * count :]
    where = place()
    greet(*where[:3])
    groups = [
        Scatter(g, far[n], near[n], line[n], totals[n], send.at[n], recv.at[n], where) for n, g in enumerate(grads)
    ]
    add = Sum(held, got, lines, small_send, small_recv, where)
    held[0] = small[...]
    add.start()
    for n in range(count + 2):
        if n < count:
            groups[n].start()
        if n == 1:
            add.step(0)
        if n == 2:
            add.step(1)
        if 1 <= n <= count:
            groups[n - 1].second()
        if n >= 2:
            groups[n - 2].third()
    add.step(2)
    for group in groups:
        group.last()
    summed[...] = add.total()
    add.finish()
    for group in groups:
        group.finish()


def scatter_all(grads, small):
    count = len(grads)
    tails = [g.shape[2:] for g in grads]
    vmem = pl.BlockSpec(memory_space=pltpu.VMEM)
    scratch = [VMEM((2, LINE) + t, jnp.bfloat16) for t in tails]
    scratch += [VMEM((LINE,) + t, jnp.bfloat16) for t in tails]
    scratch += [VMEM((3,) + t, jnp.bfloat16) for t in tails]
    scratch += [VMEM((4,) + small.shape, jnp.float32), VMEM((3,) + small.shape, jnp.float32)]
    scratch += [VMEM((LINE,) + small.shape, jnp.float32)]
    scratch += [DMA((count, 6)), DMA((count, 6)), DMA((6,)), DMA((6,))]
    return pl.pallas_call(
        functools.partial(scatter_kernel, count),
        out_shape=[jax.ShapeDtypeStruct(t, jnp.float32) for t in tails]
        + [jax.ShapeDtypeStruct(small.shape, jnp.float32)],
        in_specs=[vmem] * (count + 1),
        out_specs=[vmem] * (count + 1),
        scratch_shapes=scratch,
        compiler_params=pltpu.CompilerParams(collective_id=1, has_side_effects=True, vmem_limit_bytes=48 << 20),
        name="scatter_grads",
    )(*grads, small)


def shards_fast(
    inputs,
    w_qkv,
    qv_bias,
    w_out,
    out_bias,
    norm1_gain,
    norm1_shift,
    w_in,
    ffn_bias,
    w_down,
    down_bias,
    norm2_gain,
    norm2_shift,
    attn_drop,
    ffn_drop,
    lengths,
    cotangent,
    pooled,
    positive,
):
    views, _, local_seq, width = inputs.shape
    cores = lax.axis_size("tensor")
    seq = local_seq * cores
    columns = w_qkv.shape[2]
    heads = columns // HEAD_DIM
    f32, bf16 = jnp.float32, jnp.bfloat16
    key_ok = jnp.arange(seq)[None, :] < lengths[:, None]
    key_ok = jnp.broadcast_to(key_ok, (views, seq))
    gain_one, shift_one = norm1_gain.astype(f32), norm1_shift.astype(f32)
    gain_two, shift_two = norm2_gain.astype(f32), norm2_shift.astype(f32)
    bias_qkv = jnp.stack([qv_bias[0], jnp.zeros_like(qv_bias[0]), qv_bias[1]]).astype(f32)
    anchor, other = pooled[0], pooled[1]
    anchor = anchor * lax.rsqrt(jnp.sum(anchor * anchor, axis=-1, keepdims=True) + 1e-06)
    other = other * lax.rsqrt(jnp.sum(other * other, axis=-1, keepdims=True) + 1e-06)
    full_qkv, full_out, full_in, full_down, every = gather_all(
        w_qkv, w_out.T, w_in, w_down.T, jnp.broadcast_to(other, (8, width))
    )
    full_qkv = full_qkv.reshape(3, width, columns)
    full_out = full_out.reshape(width, -1)
    full_in = full_in.reshape(width, -1)
    full_down = full_down.reshape(width, -1)
    every = every[:, :, 0].reshape(-1, width)
    rows = inputs[:, 0]
    full_rows = lax.all_gather(rows, "tensor", axis=1, tiled=True)
    qkv = jnp.einsum("bsd,cde->cbse", full_rows, full_qkv, preferred_element_type=f32)
    qkv = (qkv + bias_qkv[:, None, None, :]).astype(bf16)
    split = qkv.reshape(3, views, seq, heads, HEAD_DIM)
    mixed, spread = attend(split[0], split[1], split[2], key_ok, seq)
    mixed = mixed.astype(bf16)
    partial_branch = jnp.einsum("bse,de->bsd", mixed, full_out, preferred_element_type=f32)

    def over_cores(partial):
        return lax.psum_scatter(partial.astype(bf16), "tensor", scatter_dimension=1, tiled=True).astype(f32)

    branch = over_cores(partial_branch) + out_bias.astype(f32)
    drop_one = attn_drop[:, 0].astype(f32) / KEEP_RATE
    first, unit_one, scale_one = normalize(rows.astype(f32) + drop_one * branch, gain_one, shift_one)
    full_first = lax.all_gather(first.astype(bf16), "tensor", axis=1, tiled=True)
    hidden = jnp.einsum("bsd,df->bsf", full_first, full_in, preferred_element_type=f32) + ffn_bias.astype(f32)
    acted = gelu_value(hidden).astype(bf16)
    partial_second = jnp.einsum("bsf,df->bsd", acted, full_down, preferred_element_type=f32)
    second = over_cores(partial_second) + down_bias.astype(f32)
    drop_two = ffn_drop[:, 0].astype(f32) / KEEP_RATE
    result, unit_two, scale_two = normalize(first + drop_two * second, gain_two, shift_two)
    grad_out = cotangent[:, 0].astype(f32)
    sum_gain_two, sum_shift_two = column_sum(grad_out * unit_two), column_sum(grad_out)
    grad_two = normalize_back(grad_out, unit_two, scale_two, gain_two)
    grad_second = (grad_two * drop_two).astype(bf16)
    sum_down = column_sum(grad_second)
    full_second = lax.all_gather(grad_second, "tensor", axis=1, tiled=True)
    grad_w_down = jnp.einsum("bsd,bsf->df", full_second, acted, preferred_element_type=f32).astype(bf16)
    grad_acted = jnp.einsum("bsd,df->bsf", full_second, full_down, preferred_element_type=f32)
    grad_hidden = (grad_acted * gelu_slope(hidden)).astype(bf16)
    grad_w_in = jnp.einsum("bsd,bsf->df", full_first, grad_hidden, preferred_element_type=f32).astype(bf16)
    sum_ffn = column_sum(grad_hidden)
    partial_first = jnp.einsum("bsf,df->bsd", grad_hidden, full_in, preferred_element_type=f32)
    grad_first = grad_two + over_cores(partial_first)
    sum_gain_one, sum_shift_one = column_sum(grad_first * unit_one), column_sum(grad_first)
    grad_one = normalize_back(grad_first, unit_one, scale_one, gain_one)
    grad_branch = (grad_one * drop_one).astype(bf16)
    sum_out = column_sum(grad_branch)
    full_branch = lax.all_gather(grad_branch, "tensor", axis=1, tiled=True)
    grad_w_out = jnp.einsum("bsd,bse->de", full_branch, mixed, preferred_element_type=f32).astype(bf16)
    grad_mixed = jnp.einsum("bsd,de->bse", full_branch, full_out, preferred_element_type=f32).astype(bf16)
    grad_query, grad_keys, grad_values = attend_back(
        split[0],
        split[1],
        split[2],
        key_ok,
        spread,
        grad_mixed.reshape(views, seq, heads, HEAD_DIM),
        seq,
    )
    grad_qkv = jnp.stack([grad_query, grad_keys, grad_values]).astype(bf16)
    grad_w_qkv = jnp.einsum("bsd,cbse->cde", full_rows, grad_qkv, preferred_element_type=f32).astype(bf16)
    sum_query, sum_value = column_sum(grad_qkv[0]), column_sum(grad_qkv[2])
    partial_rows = jnp.einsum("cbse,cde->bsd", grad_qkv, full_qkv, preferred_element_type=f32)
    grad_rows = grad_one + over_cores(partial_rows)
    logits = jnp.dot(anchor, every.T, precision=HIGH) / TEMPER
    top = jnp.max(logits, axis=-1, keepdims=True)
    log_total = top[:, 0] + jnp.log(jnp.sum(jnp.exp(logits - top), axis=-1))
    chosen = jnp.arange(every.shape[0])[None, :] == positive[:, None]
    picked = jnp.sum(jnp.where(chosen, logits, 0.0), axis=-1)
    loss_term = jnp.sum(log_total - picked)
    empty = jnp.zeros((width,), f32)
    wide = [sum_out, sum_down, sum_gain_one, sum_shift_one, sum_gain_two, sum_shift_two, empty + loss_term, empty]
    split_ffn = sum_ffn.reshape(-1, width)
    own = [jnp.concatenate([sum_query, sum_value])] + [split_ffn[i] for i in range(split_ffn.shape[0])]
    small = jnp.stack(wide + own + [empty] * (8 - len(own)))
    shape = (LINE, 4, width // (4 * LINE))
    grads = [grad_w_down, grad_w_in, grad_w_out, grad_w_qkv[0], grad_w_qkv[1], grad_w_qkv[2]]
    done = scatter_all([g.reshape(shape + (g.shape[1],)) for g in grads], small)
    total = done[-1]
    loss = total[6, 0] / (every.shape[0] * cores)
    return (
        result.astype(bf16)[:, None],
        grad_rows.astype(bf16)[:, None],
        jnp.stack(done[3:6]),
        total[8].reshape(2, -1),
        done[2].T,
        total[0],
        total[2],
        total[3],
        done[1],
        total[9 : 9 + split_ffn.shape[0]].reshape(-1),
        done[0].T,
        total[1],
        total[4],
        total[5],
        loss,
    )


def solution(mesh):
    placed = (
        P(None, "dp", "tensor", None),
        P(None, "dp", "tensor"),
        P(None, "tensor"),
        P("tensor", "dp"),
        P(),
        P(),
        P(),
        P("dp", "tensor"),
        P("tensor"),
        P("tensor", "dp"),
        P(),
        P(),
        P(),
        P(None, "dp", "tensor", None),
        P(None, "dp", "tensor", None),
        P("dp"),
        P(None, "dp", "tensor", None),
        P(None, "dp", None),
        P("dp"),
    )
    fits = mesh.shape["dp"] == 4 * LINE and mesh.shape["tensor"] == 2
    return jax.shard_map(
        shards_fast if fits else shards,
        mesh=mesh,
        in_specs=placed,
        out_specs=(
            P(None, "dp", "tensor", None),
            P(None, "dp", "tensor", None),
            P(None, "dp", "tensor"),
            P(None, "tensor"),
            P("tensor", "dp"),
            P(),
            P(),
            P(),
            P("dp", "tensor"),
            P("tensor"),
            P("tensor", "dp"),
            P(),
            P(),
            P(),
            P(),
        ),
        check_vma=False,
    )
```

```python
import functools

import jax
import jax.numpy as jnp
from jax import lax
from jax.experimental import pallas as pl
from jax.experimental.pallas import tpu as pltpu
from jax.sharding import PartitionSpec as P

HEAD_DIM = 64


KEEP_RATE = 0.9
NORM_EPS = 1e-05
TEMPER = 0.05
HIGH = lax.Precision.HIGHEST


def gelu_value(u):
    return 0.5 * u * (1.0 + jax.scipy.special.erf(u * 0.7071067811865476))


def gelu_slope(u):
    return (
        0.5 * (1.0 + jax.scipy.special.erf(u * 0.7071067811865476))
        + u * jnp.exp(-0.5 * u * u) * 0.3989422804014327
    )


def normalize(rows, gain, shift):
    centre = rows - jnp.mean(rows, axis=-1, keepdims=True)
    scale = lax.rsqrt(jnp.mean(centre * centre, axis=-1, keepdims=True) + NORM_EPS)
    unit = centre * scale
    return (unit * gain + shift, unit, scale)


def normalize_back(grad, unit, scale, gain):
    inner = grad * gain
    return scale * (
        inner
        - jnp.mean(inner, axis=-1, keepdims=True)
        - unit * jnp.mean(inner * unit, axis=-1, keepdims=True)
    )


def column_sum(values):
    return jnp.sum(values.astype(jnp.float32), axis=tuple(range(values.ndim - 1)))


def gather_weights(w_qkv, w_out, w_in, w_down):
    return (
        lax.all_gather(w_qkv, "dp", axis=1, tiled=True),
        lax.all_gather(w_out, "dp", axis=1, tiled=True),
        lax.all_gather(w_in, "dp", axis=0, tiled=True),
        lax.all_gather(w_down, "dp", axis=1, tiled=True),
    )


def attend(query, keys, values, key_ok, block):
    sents, seq, heads, width = query.shape
    count = seq // block
    q_blocks = jnp.moveaxis(query.reshape(sents, count, block, heads, width), 1, 0)

    def one_block(q_block):
        scores = (
            jnp.einsum("bqhd,bkhd->bhqk", q_block, keys, preferred_element_type=jnp.float32) * 0.125
        )
        scores = jnp.where(key_ok[:, None, None, :], scores, -1e30)
        top = jnp.max(scores, axis=-1, keepdims=True)
        raised = jnp.exp(scores - top)
        total = jnp.sum(raised, axis=-1, keepdims=True)
        probs = (raised / total).astype(jnp.bfloat16)
        mixed = jnp.einsum("bhqk,bkhd->bqhd", probs, values, preferred_element_type=jnp.float32)
        return (mixed, top[..., 0] + jnp.log(total[..., 0]))

    mixed, spread = lax.map(one_block, q_blocks)
    mixed = jnp.moveaxis(mixed, 0, 1).reshape(sents, seq, heads * width)
    return (mixed, spread)


def attend_back(query, keys, values, key_ok, spread, grad_mixed, block):
    sents, seq, heads, width = query.shape
    count = seq // block
    q_blocks = jnp.moveaxis(query.reshape(sents, count, block, heads, width), 1, 0)
    g_blocks = jnp.moveaxis(grad_mixed.reshape(sents, count, block, heads, width), 1, 0)

    def one_block(carry, item):
        grad_keys, grad_values = carry
        q_block, g_block, s_block = item
        scores = (
            jnp.einsum("bqhd,bkhd->bhqk", q_block, keys, preferred_element_type=jnp.float32) * 0.125
        )
        scores = jnp.where(key_ok[:, None, None, :], scores, -1e30)
        probs = jnp.exp(scores - s_block[..., None])
        grad_probs = jnp.einsum(
            "bqhd,bkhd->bhqk", g_block, values, preferred_element_type=jnp.float32
        )
        grad_scores = (
            probs * (grad_probs - jnp.sum(probs * grad_probs, axis=-1, keepdims=True))
        ).astype(jnp.bfloat16)
        grad_query = (
            jnp.einsum("bhqk,bkhd->bqhd", grad_scores, keys, preferred_element_type=jnp.float32)
            * 0.125
        )
        grad_keys = (
            grad_keys
            + jnp.einsum(
                "bhqk,bqhd->bkhd", grad_scores, q_block, preferred_element_type=jnp.float32
            )
            * 0.125
        )
        grad_values = grad_values + jnp.einsum(
            "bhqk,bqhd->bkhd",
            probs.astype(jnp.bfloat16),
            g_block,
            preferred_element_type=jnp.float32,
        )
        return ((grad_keys, grad_values), grad_query)

    zero = jnp.zeros((sents, seq, heads, width), jnp.float32)
    (grad_keys, grad_values), grad_query = lax.scan(
        one_block, (zero, zero), (q_blocks, g_blocks, spread)
    )
    grad_query = jnp.moveaxis(grad_query, 0, 1).reshape(sents, seq, heads * width)
    return (
        grad_query,
        grad_keys.reshape(sents, seq, heads * width),
        grad_values.reshape(sents, seq, heads * width),
    )


def shards(
    inputs,
    w_qkv,
    qv_bias,
    w_out,
    out_bias,
    norm1_gain,
    norm1_shift,
    w_in,
    ffn_bias,
    w_down,
    down_bias,
    norm2_gain,
    norm2_shift,
    attn_drop,
    ffn_drop,
    lengths,
    cotangent,
    pooled,
    positive,
):
    views, sents, local_seq, width = inputs.shape
    seq = local_seq * lax.axis_size("tensor")
    block = min(512, seq)
    heads = w_qkv.shape[2] // HEAD_DIM
    key_ok = jnp.arange(seq)[None, :] < lengths[:, None]
    gain_one = norm1_gain.astype(jnp.float32)
    shift_one = norm1_shift.astype(jnp.float32)
    gain_two = norm2_gain.astype(jnp.float32)
    shift_two = norm2_shift.astype(jnp.float32)
    bias_out = out_bias.astype(jnp.float32)
    bias_down = down_bias.astype(jnp.float32)
    bias_ffn = ffn_bias.astype(jnp.float32)
    bias_qkv = jnp.stack([qv_bias[0], jnp.zeros_like(qv_bias[0]), qv_bias[1]]).astype(jnp.float32)
    shard_grads = tuple((jnp.zeros(w.shape, jnp.float32) for w in (w_qkv, w_out, w_in, w_down)))
    acc_gain_one = jnp.zeros((width,), jnp.float32)
    acc_shift_one = jnp.zeros((width,), jnp.float32)
    acc_gain_two = jnp.zeros((width,), jnp.float32)
    acc_shift_two = jnp.zeros((width,), jnp.float32)
    acc_out_bias = jnp.zeros((width,), jnp.float32)
    acc_down_bias = jnp.zeros((width,), jnp.float32)
    acc_ffn_bias = jnp.zeros(ffn_bias.shape, jnp.float32)
    acc_qv_bias = jnp.zeros(qv_bias.shape, jnp.float32)
    outputs = []
    input_grads = []
    for view in range(views):
        whole = gather_weights(w_qkv, w_out, w_in, w_down)
        full_qkv, full_out, full_in, full_down = whole
        rows = inputs[view]
        full_rows = lax.all_gather(rows, "tensor", axis=1, tiled=True)
        qkv = jnp.einsum("bsd,cde->cbse", full_rows, full_qkv, preferred_element_type=jnp.float32)
        qkv = (qkv + bias_qkv[:, None, None, :]).astype(jnp.bfloat16)
        split = qkv.reshape(3, sents, seq, heads, HEAD_DIM)
        mixed, spread = attend(split[0], split[1], split[2], key_ok, block)
        mixed = mixed.astype(jnp.bfloat16)
        partial_branch = jnp.einsum(
            "bse,ed->bsd", mixed, full_out, preferred_element_type=jnp.float32
        )
        branch = (
            lax.psum_scatter(
                partial_branch.astype(jnp.bfloat16), "tensor", scatter_dimension=1, tiled=True
            ).astype(jnp.float32)
            + bias_out
        )
        drop_one = attn_drop[view].astype(jnp.float32) / KEEP_RATE
        first, unit_one, scale_one = normalize(
            rows.astype(jnp.float32) + drop_one * branch, gain_one, shift_one
        )
        full_first = lax.all_gather(first.astype(jnp.bfloat16), "tensor", axis=1, tiled=True)
        hidden = (
            jnp.einsum("bsd,df->bsf", full_first, full_in, preferred_element_type=jnp.float32)
            + bias_ffn
        )
        acted = gelu_value(hidden).astype(jnp.bfloat16)
        partial_second = jnp.einsum(
            "bsf,fd->bsd", acted, full_down, preferred_element_type=jnp.float32
        )
        second = (
            lax.psum_scatter(
                partial_second.astype(jnp.bfloat16), "tensor", scatter_dimension=1, tiled=True
            ).astype(jnp.float32)
            + bias_down
        )
        drop_two = ffn_drop[view].astype(jnp.float32) / KEEP_RATE
        result, unit_two, scale_two = normalize(first + drop_two * second, gain_two, shift_two)
        outputs.append(result.astype(jnp.bfloat16))
        full_qkv, full_out, full_in, full_down = gather_weights(w_qkv, w_out, w_in, w_down)
        grad_out = cotangent[view].astype(jnp.float32)
        acc_gain_two = acc_gain_two + column_sum(grad_out * unit_two)
        acc_shift_two = acc_shift_two + column_sum(grad_out)
        grad_two = normalize_back(grad_out, unit_two, scale_two, gain_two)
        grad_second = (grad_two * drop_two).astype(jnp.bfloat16)
        full_second = lax.all_gather(grad_second, "tensor", axis=1, tiled=True)
        grad_w_down = jnp.einsum(
            "bsf,bsd->fd", acted, full_second, preferred_element_type=jnp.float32
        )
        acc_down_bias = acc_down_bias + column_sum(full_second)
        grad_acted = jnp.einsum(
            "bsd,fd->bsf", full_second, full_down, preferred_element_type=jnp.float32
        )
        grad_hidden = (grad_acted * gelu_slope(hidden)).astype(jnp.bfloat16)
        grad_w_in = jnp.einsum(
            "bsd,bsf->df", full_first, grad_hidden, preferred_element_type=jnp.float32
        )
        acc_ffn_bias = acc_ffn_bias + column_sum(grad_hidden)
        partial_first = jnp.einsum(
            "bsf,df->bsd", grad_hidden, full_in, preferred_element_type=jnp.float32
        )
        grad_first = grad_two + lax.psum_scatter(
            partial_first.astype(jnp.bfloat16), "tensor", scatter_dimension=1, tiled=True
        ).astype(jnp.float32)
        acc_gain_one = acc_gain_one + column_sum(grad_first * unit_one)
        acc_shift_one = acc_shift_one + column_sum(grad_first)
        grad_one = normalize_back(grad_first, unit_one, scale_one, gain_one)
        grad_branch = (grad_one * drop_one).astype(jnp.bfloat16)
        full_branch = lax.all_gather(grad_branch, "tensor", axis=1, tiled=True)
        grad_w_out = jnp.einsum(
            "bse,bsd->ed", mixed, full_branch, preferred_element_type=jnp.float32
        )
        acc_out_bias = acc_out_bias + column_sum(full_branch)
        grad_mixed = jnp.einsum(
            "bsd,ed->bse", full_branch, full_out, preferred_element_type=jnp.float32
        ).astype(jnp.bfloat16)
        grad_query, grad_keys, grad_values = attend_back(
            split[0],
            split[1],
            split[2],
            key_ok,
            spread,
            grad_mixed.reshape(sents, seq, heads, HEAD_DIM),
            block,
        )
        grad_qkv = jnp.stack([grad_query, grad_keys, grad_values]).astype(jnp.bfloat16)
        grad_w_qkv = jnp.einsum(
            "bsd,cbse->cde", full_rows, grad_qkv, preferred_element_type=jnp.float32
        )
        acc_qv_bias = acc_qv_bias + jnp.stack([column_sum(grad_qkv[0]), column_sum(grad_qkv[2])])
        partial_rows = jnp.einsum(
            "cbse,cde->bsd", grad_qkv, full_qkv, preferred_element_type=jnp.float32
        )
        grad_rows = grad_one + lax.psum_scatter(
            partial_rows.astype(jnp.bfloat16), "tensor", scatter_dimension=1, tiled=True
        ).astype(jnp.float32)
        input_grads.append(grad_rows.astype(jnp.bfloat16))
        local_grads = (grad_w_qkv, grad_w_out, grad_w_in, grad_w_down)
        summed = (
            lax.psum_scatter(local_grads[0], "dp", scatter_dimension=1, tiled=True),
            lax.psum_scatter(local_grads[1], "dp", scatter_dimension=1, tiled=True),
            lax.psum_scatter(local_grads[2], "dp", scatter_dimension=0, tiled=True),
            lax.psum_scatter(local_grads[3], "dp", scatter_dimension=1, tiled=True),
        )
        shard_grads = tuple((a + b for a, b in zip(shard_grads, summed)))
    anchor = pooled[0]
    other = pooled[1]
    anchor = anchor * lax.rsqrt(jnp.sum(anchor * anchor, axis=-1, keepdims=True) + 1e-06)
    other = other * lax.rsqrt(jnp.sum(other * other, axis=-1, keepdims=True) + 1e-06)
    every = lax.all_gather(other, "dp", axis=0, tiled=True)
    logits = jnp.dot(anchor, every.T, precision=HIGH) / TEMPER
    top = jnp.max(logits, axis=-1, keepdims=True)
    log_total = top[:, 0] + jnp.log(jnp.sum(jnp.exp(logits - top), axis=-1))
    chosen = jnp.arange(every.shape[0])[None, :] == positive[:, None]
    picked = jnp.sum(jnp.where(chosen, logits, 0.0), axis=-1)
    loss_term = jnp.sum(log_total - picked)
    sum_qv, sum_out, sum_ffn, sum_down = lax.psum(
        (acc_qv_bias, acc_out_bias, acc_ffn_bias, acc_down_bias), "dp"
    )
    sum_gain_one, sum_shift_one, sum_gain_two, sum_shift_two, loss_sum = lax.psum(
        (acc_gain_one, acc_shift_one, acc_gain_two, acc_shift_two, loss_term), ("dp", "tensor")
    )
    loss = loss_sum / (every.shape[0] * lax.axis_size("tensor"))
    return (
        jnp.stack(outputs),
        jnp.stack(input_grads),
        shard_grads[0],
        sum_qv,
        shard_grads[1],
        sum_out,
        sum_gain_one,
        sum_shift_one,
        shard_grads[2],
        sum_ffn,
        shard_grads[3],
        sum_down,
        sum_gain_two,
        sum_shift_two,
        loss,
    )


MESH = pl.DeviceIdType.MESH
VMEM = pltpu.VMEM
DMA = pltpu.SemaphoreType.DMA
LINE = 4


def place():
    me = lax.axis_index("dp")
    core = lax.axis_index("tensor")
    z, q = me // 4, me % 4
    y, x = q // 2, q % 2
    over_y, over_x = (1 - y) * 2 + x, y * 2 + 1 - x
    near = (1 - core) * over_y + core * over_x
    far = core * over_y + (1 - core) * over_x
    return z, q, core, near, far, 3 - q


def greet(z, q, core):
    barrier = pltpu.get_barrier_semaphore()
    peers = [((z + k) % LINE * 4 + q, core) for k in (1, 2, 3)]
    y, x = q // 2, q % 2
    peers += [(z * 4 + (1 - y) * 2 + x, core), (z * 4 + y * 2 + 1 - x, core), (z * 4 + q, 1 - core)]
    for peer in peers:
        pl.semaphore_signal(barrier, inc=1, device_id=peer, device_id_type=MESH)
    pl.semaphore_wait(barrier, len(peers))


def remote(src, dst, send, recv, device):
    return pltpu.make_async_remote_copy(
        src_ref=src, dst_ref=dst, send_sem=send, recv_sem=recv, device_id=device, device_id_type=MESH
    )


class Gather:
    def __init__(self, shard, whole, send, recv, local, at, where):
        self.shard, self.whole, self.send, self.recv, self.local, self.at = shard, whole, send, recv, local, at
        self.where = where

    def part(self, z, q):
        return self.whole.at[self.at + (z, q)]

    def line(self, q):
        return self.whole.at[self.at + (slice(None), q)]

    def start(self):
        z, q, core, near, far, corner = self.where
        self.own = pltpu.make_async_copy(self.shard, self.part(z, q), self.local)
        self.own.start()
        self.along = []
        for k in (1, 3, 2):
            copy = remote(
                self.shard, self.part(z, q), self.send.at[k - 1], self.recv.at[k - 1], ((z + k) % LINE * 4 + q, core)
            )
            copy.start()
            self.along.append(copy)

    def spread(self):
        z, q, core, near, far, corner = self.where
        for copy in self.along:
            copy.wait_recv()
        self.own.wait()
        self.to_near = remote(self.line(q), self.line(q), self.send.at[3], self.recv.at[3], (z * 4 + near, core))
        self.to_far = remote(self.line(q), self.line(q), self.send.at[4], self.recv.at[4], (z * 4 + far, core))
        self.to_near.start()
        self.to_far.start()

    def forward(self):
        z, q, core, near, far, corner = self.where
        self.to_near.wait_recv()
        self.pass_on = remote(self.line(near), self.line(near), self.send.at[5], self.recv.at[5], (z * 4 + far, core))
        self.pass_on.start()

    def ready(self):
        self.to_far.wait_recv()
        self.pass_on.wait_recv()

    def finish(self):
        for copy in self.along + [self.to_near, self.to_far, self.pass_on]:
            copy.wait_send()


class Scatter:
    def __init__(self, grad, got_far, got_near, got_line, total, send, recv, where):
        self.grad, self.got_far, self.got_near, self.got_line = grad, got_far, got_near, got_line
        self.total, self.send, self.recv, self.where = total, send, recv, where

    def start(self):
        z, q, core, near, far, corner = self.where
        there = (z * 4 + far, core)
        self.far_own = remote(self.grad.at[:, far], self.got_far.at[0], self.send.at[0], self.recv.at[0], there)
        self.far_near = remote(self.grad.at[:, corner], self.got_far.at[1], self.send.at[1], self.recv.at[1], there)
        self.far_near.start()
        self.far_own.start()

    def second(self):
        z, q, core, near, far, corner = self.where
        self.far_near.wait_recv()

        def add(i, carry):
            self.grad[i, near] = (
                self.grad[i, near].astype(jnp.float32) + self.got_far[1, i].astype(jnp.float32)
            ).astype(jnp.bfloat16)
            return carry

        lax.fori_loop(0, LINE, add, 0)
        self.to_near = remote(
            self.grad.at[:, near], self.got_near, self.send.at[2], self.recv.at[2], (z * 4 + near, core)
        )
        self.to_near.start()

    def third(self):
        z, q, core, near, far, corner = self.where
        self.far_own.wait_recv()
        self.to_near.wait_recv()

        def sum_of(i):
            return (
                self.grad[i, q].astype(jnp.float32)
                + self.got_far[0, i].astype(jnp.float32)
                + self.got_near[i].astype(jnp.float32)
            )

        self.total[...] = sum_of(z)

        def add(i, carry):
            self.grad[i, q] = sum_of(i).astype(jnp.bfloat16)
            return carry

        lax.fori_loop(0, LINE, add, 0)
        self.along = []
        for k in (1, 3, 2):
            there = (z + k) % LINE
            copy = remote(
                self.grad.at[there, q], self.got_line.at[k - 1], self.send.at[2 + k], self.recv.at[2 + k],
                (there * 4 + q, core),
            )
            copy.start()
            self.along.append(copy)

    def last(self):
        for copy in self.along:
            copy.wait_recv()
        total = self.total[...]
        for k in range(3):
            total = total + self.got_line[k].astype(jnp.float32)
        self.total[...] = total

    def finish(self):
        for copy in self.along + [self.far_own, self.far_near, self.to_near]:
            copy.wait_send()


class Sum:
    def __init__(self, held, got, lines, send, recv, where):
        self.held, self.got, self.lines, self.send, self.recv, self.where = held, got, lines, send, recv, where

    def hop(self, n, device, rows):
        copy = remote(
            self.held.at[n, pl.ds(0, rows)], self.got.at[n, pl.ds(0, rows)], self.send.at[n], self.recv.at[n], device
        )
        copy.start()
        self.copy = copy

    def start(self):
        z, q, core, near, far, corner = self.where
        self.copies = []
        self.hop(0, (z * 4 + q, 1 - core), 8)

    def step(self, n):
        z, q, core, near, far, corner = self.where
        y, x = q // 2, q % 2
        self.copy.wait_recv()
        self.copies.append(self.copy)
        rows = self.held.shape[1]
        if n == 0:
            self.held[1, :8] = self.held[0, :8] + self.got[0, :8]
            self.held[1, 8:] = self.held[0, 8:]
            self.hop(1, (z * 4 + y * 2 + 1 - x, core), rows)
        elif n == 1:
            self.held[2] = self.held[1] + self.got[1]
            self.hop(2, (z * 4 + (1 - y) * 2 + x, core), rows)
        else:
            total = self.held[2] + self.got[2]
            self.held[3] = total
            self.lines[z] = total
            for k in (1, 2, 3):
                there = (z + k) % LINE
                copy = remote(
                    self.held.at[3], self.lines.at[z], self.send.at[2 + k], self.recv.at[2 + k], (there * 4 + q, core)
                )
                copy.start()
                self.copies.append(copy)

    def total(self):
        for copy in self.copies[3:]:
            copy.wait_recv()
        return (self.lines[0] + self.lines[1]) + (self.lines[2] + self.lines[3])

    def finish(self):
        for copy in self.copies:
            copy.wait_send()


def nt(a, b):
    return lax.dot_general(a, b, (((1,), (1,)), ((), ())), preferred_element_type=jnp.float32)


def tn(a, b):
    return lax.dot_general(a, b, (((0,), (0,)), ((), ())), preferred_element_type=jnp.float32)


def nn(a, b):
    return jnp.dot(a, b, preferred_element_type=jnp.float32)


STEP_ROWS = 64


def step_kernel(*refs):
    f32, bf16 = jnp.float32, jnp.bfloat16
    (
        x_hbm, attn_hbm, ffn_hbm, cot_hbm,
        s_qkv, s_out, s_in, s_down, qv_bias, b_out, b_ffn, b_down, gains, pooled, lengths, positive,
        y_out, dx_out, o_qkv, o_out, o_in, o_down, o_small,
        w_qkv, w_out, w_in, w_down, w_pool, own_pool,
        rows_x, qkv, spread, mixed, send_buf, got_buf, own_buf, first, unit, scale,
        full_first, acted, slope, grad_two, full_second, full_branch, grad_mixed, grad_qkv,
        drop_one, drop_two, cot, grads_wide, grads_thin, far_wide, far_thin, near_wide, near_thin, line_wide, line_thin,
        held, got_small, lines_small,
        ag_send, ag_recv, ag_local, rs_send, rs_recv, sum_send, sum_recv, tp_send, tp_recv, load_sem,
    ) = refs
    where = place()
    z, q, core, near, far, corner = where
    half = 256
    width = 768
    cols = 384
    other = 1 - core
    partner = (z * 4 + q, other)

    loads = [
        pltpu.make_async_copy(x_hbm, rows_x.at[:, core], load_sem.at[0]),
        pltpu.make_async_copy(attn_hbm, drop_one, load_sem.at[1]),
        pltpu.make_async_copy(ffn_hbm, drop_two, load_sem.at[2]),
        pltpu.make_async_copy(cot_hbm, cot, load_sem.at[3]),
    ]
    for load in loads:
        load.start()
    greet(z, q, core)

    anchor, pair = pooled[0], pooled[1]
    anchor = anchor * lax.rsqrt(jnp.sum(anchor * anchor, axis=-1, keepdims=True) + 1e-06)
    pair = pair * lax.rsqrt(jnp.sum(pair * pair, axis=-1, keepdims=True) + 1e-06)
    own_pool[...] = jnp.broadcast_to(pair, own_pool.shape)

    pairs = [(s_qkv.at[i], w_qkv, (i,)) for i in range(3)]
    pairs += [(s_out, w_out, ())]
    pairs += [(s_in.at[:, pl.ds(h * width, width)], w_in, (h,)) for h in range(2)]
    pairs += [(s_down.at[:, pl.ds(h * width, width)], w_down, (h,)) for h in range(2)]
    pairs += [(own_pool, w_pool, ())]
    groups = [
        Gather(s, w, ag_send.at[n], ag_recv.at[n], ag_local.at[n], at, where) for n, (s, w, at) in enumerate(pairs)
    ]
    g_q, g_k, g_v, g_out, g_in0, g_in1, g_down0, g_down1, g_pool = groups
    order = [g_q, g_k, g_v, g_out, g_pool, g_in0, g_in1, g_down0, g_down1]
    for group in order[:3]:
        group.start()

    pending = []

    def send(kind, view, src, dst):
        copy = remote(src, dst, tp_send.at[kind, view], tp_recv.at[kind, view], partner)
        copy.start()
        if kind not in (1, 3, 5):
            pending.append(copy)
        return copy

    loads[0].wait()
    x_copies = [send(0, v, rows_x.at[v, core], rows_x.at[v, core]) for v in range(2)]
    for group in order[3:]:
        group.start()

    held[0] = jnp.zeros(held.shape[1:], f32)

    def flat(w):
        return w.reshape(width, w.shape[-1])

    for group in (g_q, g_k, g_v):
        group.spread()
    for group in (g_q, g_k, g_v):
        group.forward()
    g_out.spread()
    g_pool.spread()
    for copy in x_copies:
        copy.wait_recv()
    for group in (g_q, g_k, g_v):
        group.ready()

    def project(v):
        def block(h, carry):
            rows = rows_x[v, h]
            at = pl.ds(pl.multiple_of(h * half, half), half)
            qkv[0, v, at] = ((nn(rows, flat(w_qkv[0])) + qv_bias[0:1].astype(f32)).astype(bf16) * 0.125).astype(bf16)
            qkv[1, v, at] = nn(rows, flat(w_qkv[1])).astype(bf16)
            qkv[2, v, at] = (nn(rows, flat(w_qkv[2])) + qv_bias[1:2].astype(f32)).astype(bf16)
            return carry

        lax.fori_loop(0, 2, block, 0)

    project(0)
    g_out.forward()
    g_pool.forward()
    g_in0.spread()
    project(1)

    key_at = lax.broadcasted_iota(jnp.int32, (2 * half, 1), 0)
    key_bias = jnp.where(key_at < lengths[0], 0.0, -1e30)
    lane = lax.broadcasted_iota(jnp.int32, (2 * half, 128), 1)

    def only(values, head):
        return jnp.where((lane < 64) == (head == 0), values, jnp.zeros_like(values))

    def attention(v):
        def one_pair(p, carry):
            at = pl.ds(pl.multiple_of(p * 128, 128), 128)
            query, keys, values = qkv[0, v, :, at], qkv[1, v, :, at], qkv[2, v, :, at]
            values_t = values.T
            outs = []
            for head in range(2):
                scores = nt(keys, only(query, head)) + key_bias
                top = jnp.max(scores, axis=0, keepdims=True)
                raised = jnp.exp(scores - top)
                total = jnp.sum(raised, axis=0, keepdims=True)
                spread[v * 3 + p, head : head + 1] = top + jnp.log(total)
                probs = (raised * (1.0 / total)).astype(bf16)
                outs.append(nn(values_t[head * 64 : head * 64 + 64], probs).astype(bf16))
            mixed[v, :, at] = jnp.concatenate(outs, axis=0).T
            return carry

        lax.fori_loop(0, 3, one_pair, 0)

    attention(0)
    g_in0.forward()
    g_in1.spread()
    attention(1)
    g_out.ready()
    g_in1.forward()

    def halves(ref, v, h):
        return ref[v, pl.ds(pl.multiple_of(h * half, half), half)]

    def branch_of(v, h):
        return nt(halves(mixed, v, h), flat(w_out[...]))

    got_a = []
    for v in range(2):
        send_buf[v] = branch_of(v, other).astype(bf16)
        got_a.append(send(1, v, send_buf.at[v], got_buf.at[v]))
    for v in range(2):
        own_buf[v] = branch_of(v, core)
    g_down0.spread()
    loads[1].wait()

    gain_one, shift_one = gains[0:1].astype(f32), gains[1:2].astype(f32)
    gain_two, shift_two = gains[2:3].astype(f32), gains[3:4].astype(f32)
    keep = 1.0 / KEEP_RATE
    inv = 1.0 / width

    def mean(values):
        return jnp.sum(values, axis=-1, keepdims=True) * inv

    def pieces(body):
        def step(i, carry):
            body(pl.ds(pl.multiple_of(i * STEP_ROWS, STEP_ROWS), STEP_ROWS))
            return carry

        lax.fori_loop(0, half // STEP_ROWS, step, 0)

    def norm_one(v):
        bias = b_out[...].astype(f32)

        def body(at):
            x = rows_x[v, core, at].astype(f32)
            branch = own_buf[v, at] + got_buf[v, at].astype(f32) + bias
            r = x + drop_one[v, at].astype(f32) * keep * branch
            centre = r - mean(r)
            sc = lax.rsqrt(mean(centre * centre) + NORM_EPS)
            un = centre * sc
            h = un * gain_one + shift_one
            unit[v, at] = un
            scale[v, at] = sc
            first[v, at] = h
            full_first[v, core, at] = h.astype(bf16)

        pieces(body)

    h_copies = []
    for v in range(2):
        got_a[v].wait_recv()
        norm_one(v)
        h_copies.append(send(2, v, full_first.at[v, core], full_first.at[v, core]))
    g_in0.ready()
    g_down0.forward()

    def hidden_block(v, h, part):
        rows = full_first[v, h]
        for n in range(2):
            at = pl.ds(n * cols, cols)
            w = w_in[part, :, :, :, at].reshape(width, cols)
            u = nn(rows, w) + b_ffn[part : part + 1, at].astype(f32)
            phi = 0.5 + 0.5 * lax.erf(u * 0.7071067811865476)
            acted[part, v, h, :, at] = (u * phi).astype(bf16)
            slope[part, v, h, :, at] = (phi + u * jnp.exp(-0.5 * u * u) * 0.3989422804014327).astype(bf16)

    def hidden(h, part):
        def body(v, carry):
            hidden_block(v, h, part)
            return carry

        lax.fori_loop(0, 2, body, 0)

    hidden(core, 0)
    g_in1.ready()
    g_down1.spread()
    hidden(core, 1)
    for copy in h_copies:
        copy.wait_recv()
    g_down1.forward()
    hidden(other, 0)
    hidden(other, 1)
    g_down0.ready()
    g_down1.ready()

    def second_of(v, h):
        return nt(acted[0, v, h], flat(w_down[0])) + nt(acted[1, v, h], flat(w_down[1]))

    got_f = []
    for v in range(2):
        got_a[v].wait_send()
        send_buf[v] = second_of(v, other).astype(bf16)
        got_f.append(send(3, v, send_buf.at[v], got_buf.at[v]))
    for v in range(2):
        own_buf[v] = second_of(v, core)
    loads[2].wait()
    loads[3].wait()

    def add_rows(row, values):
        held[0, row : row + 1] += jnp.sum(values, axis=0, keepdims=True)

    def norm_two(v):
        bias = b_down[...].astype(f32)

        def body(at):
            drop = drop_two[v, at].astype(f32) * keep
            r = first[v, at] + drop * (own_buf[v, at] + got_buf[v, at].astype(f32) + bias)
            centre = r - mean(r)
            sc = lax.rsqrt(mean(centre * centre) + NORM_EPS)
            un = centre * sc
            y_out[v, at] = (un * gain_two + shift_two).astype(bf16)
            dy = cot[v, at].astype(f32)
            add_rows(4, dy * un)
            add_rows(5, dy)
            e = dy * gain_two
            d = sc * (e - mean(e) - un * mean(e * un))
            grad_two[v, at] = d
            df = (d * drop).astype(bf16)
            add_rows(1, df.astype(f32))
            full_second[v, core, at] = df

        pieces(body)

    df_copies = []
    for v in range(2):
        got_f[v].wait_recv()
        norm_two(v)
        df_copies.append(send(4, v, full_second.at[v, core], full_second.at[v, core]))

    def hidden_back(h):
        def body(i, carry):
            part, v = i // 2, i % 2
            rows = full_second[v, h]
            for n in range(2):
                at = pl.ds(n * cols, cols)
                d = nn(rows, w_down[part, :, :, :, at].reshape(width, cols))
                du = (d * slope[part, v, h, :, at].astype(f32)).astype(bf16)
                slope[part, v, h, :, at] = du
                lines_ffn = jnp.sum(du.astype(f32), axis=0, keepdims=True)
                held[0, pl.ds(9 + part, 1), at] += lines_ffn
            return carry

        lax.fori_loop(0, 4, body, 0)

    hidden_back(core)
    for copy in df_copies:
        copy.wait_recv()

    def weight_grad(out, left, right):
        def body(i, carry):
            at = pl.ds(pl.multiple_of(i * cols, cols), cols)
            value = tn(left(at), right()).astype(bf16)
            out[pl.ds(i * 2, 2)] = value.reshape(2, 4, 48, value.shape[-1])
            return carry

        lax.fori_loop(0, 2, body, 0)

    def of(ref):
        return lambda at: ref[:, :, :, at].reshape(4 * half, cols)

    totals = [
        o_down.at[:, pl.ds(0, width)], o_down.at[:, pl.ds(width, width)],
        o_in.at[:, pl.ds(0, width)], o_in.at[:, pl.ds(width, width)],
        o_out, o_qkv.at[0], o_qkv.at[1], o_qkv.at[2],
    ]
    sums = []
    for n in range(8):
        if n < 4:
            bufs = (grads_wide.at[n], far_wide.at[n], near_wide.at[n], line_wide.at[n])
        else:
            bufs = (grads_thin.at[n - 4], far_thin.at[n - 4], near_thin.at[n - 4], line_thin.at[n - 4])
        sums.append(Scatter(*bufs, totals[n], rs_send.at[n], rs_recv.at[n], where))

    for part in range(2):
        weight_grad(grads_wide.at[part], of(full_second), lambda: acted[part].reshape(4 * half, width))
        sums[part].start()
    hidden_back(other)

    def first_of(v, h):
        return nt(slope[0, v, h], flat(w_in[0])) + nt(slope[1, v, h], flat(w_in[1]))

    got_h = []
    for v in range(2):
        got_f[v].wait_send()
        send_buf[v] = first_of(v, other).astype(bf16)
        got_h.append(send(5, v, send_buf.at[v], got_buf.at[v]))
    sums[0].second()
    for v in range(2):
        own_buf[v] = first_of(v, core)
    sums[1].second()

    def norm_one_back(v):
        def body(at):
            un = unit[v, at]
            dh = grad_two[v, at] + own_buf[v, at] + got_buf[v, at].astype(f32)
            add_rows(2, dh * un)
            add_rows(3, dh)
            e = dh * gain_one
            d = scale[v, at] * (e - mean(e) - un * mean(e * un))
            grad_two[v, at] = d
            da = (d * (drop_one[v, at].astype(f32) * keep)).astype(bf16)
            add_rows(0, da.astype(f32))
            full_branch[v, core, at] = da

        pieces(body)

    da_copies = []
    for v in range(2):
        got_h[v].wait_recv()
        norm_one_back(v)
        da_copies.append(send(6, v, full_branch.at[v, core], full_branch.at[v, core]))
    weight_grad(grads_wide.at[2], of(full_first), lambda: slope[0].reshape(4 * half, width))
    sums[2].start()
    sums[0].third()
    weight_grad(grads_wide.at[3], of(full_first), lambda: slope[1].reshape(4 * half, width))
    sums[3].start()
    sums[1].third()

    for copy in da_copies:
        copy.wait_recv()

    def mixed_back(i, carry):
        v, h = i // 2, i % 2
        at = pl.ds(pl.multiple_of(h * half, half), half)
        grad_mixed[v, at] = nn(full_branch[v, h], flat(w_out[...])).astype(bf16)
        return carry

    lax.fori_loop(0, 4, mixed_back, 0)
    weight_grad(grads_thin.at[0], of(full_branch), lambda: mixed[...].reshape(4 * half, cols))
    sums[4].start()
    sums[2].second()

    def attention_back(v):
        def one_pair(p, carry):
            at = pl.ds(pl.multiple_of(p * 128, 128), 128)
            query, keys, values = qkv[0, v, :, at], qkv[1, v, :, at], qkv[2, v, :, at]
            grad_out = grad_mixed[v, :, at]
            keys_t = keys.T
            dq, dk, dv = [], 0.0, 0.0
            for head in range(2):
                own_query, own_out = only(query, head), only(grad_out, head)
                scores = nt(keys, own_query) + key_bias
                probs = jnp.exp(scores - spread[v * 3 + p, head : head + 1])
                dp = nt(values, own_out)
                ds = (probs * (dp - jnp.sum(probs * dp, axis=0, keepdims=True))).astype(bf16)
                dv = dv + nn(probs.astype(bf16), own_out)
                dk = dk + nn(ds, own_query)
                dq.append(nn(keys_t[head * 64 : head * 64 + 64], ds) * 0.125)
            dq = jnp.concatenate([d.astype(bf16) for d in dq], axis=0).T
            dv = dv.astype(bf16)
            grad_qkv[0, v, :, at] = dq
            grad_qkv[1, v, :, at] = dk.astype(bf16)
            grad_qkv[2, v, :, at] = dv
            held[0, 8:9, at] += jnp.sum(dq.astype(f32), axis=0, keepdims=True)
            at_v = pl.ds(pl.multiple_of(cols + p * 128, 128), 128)
            held[0, 8:9, at_v] += jnp.sum(dv.astype(f32), axis=0, keepdims=True)
            return carry

        lax.fori_loop(0, 3, one_pair, 0)

    attention_back(0)
    sums[3].second()
    sums[2].third()
    sums[4].second()
    attention_back(1)
    sums[3].third()
    sums[4].third()

    g_pool.ready()
    every = w_pool[...].reshape(LINE * 4, 8, width)[:, 0]
    logits = jnp.sum(every * anchor, axis=-1, keepdims=True) * (1.0 / TEMPER)
    top = jnp.max(logits, axis=0, keepdims=True)
    log_total = top + jnp.log(jnp.sum(jnp.exp(logits - top), axis=0, keepdims=True))
    chosen = lax.broadcasted_iota(jnp.int32, logits.shape, 0) == positive[0]
    picked = jnp.sum(jnp.where(chosen, logits, 0.0), axis=0, keepdims=True)
    held[0, 6:7] = jnp.broadcast_to(log_total - picked, (1, width))
    add = Sum(held, got_small, lines_small, sum_send, sum_recv, where)
    add.start()

    for c in range(3):
        weight_grad(grads_thin.at[1 + c], of(rows_x), lambda: grad_qkv[c].reshape(4 * half, cols))
        sums[5 + c].start()
        if c == 0:
            add.step(0)
    add.step(1)

    def rows_of(v, h):
        at = pl.ds(pl.multiple_of(h * half, half), half)
        return sum(nt(grad_qkv[c, v, at], flat(w_qkv[c])) for c in range(3))

    got_x = []
    for v in range(2):
        got_h[v].wait_send()
        send_buf[v] = rows_of(v, other).astype(bf16)
        got_x.append(send(7, v, send_buf.at[v], got_buf.at[v]))
    sums[5].second()
    for v in range(2):
        own_buf[v] = rows_of(v, core)
    sums[6].second()
    add.step(2)
    sums[7].second()
    for n in range(4):
        sums[n].last()
    sums[5].third()
    for v in range(2):
        got_x[v].wait_recv()

        def body(at):
            dx_out[v, at] = (grad_two[v, at] + own_buf[v, at] + got_buf[v, at].astype(f32)).astype(bf16)

        pieces(body)
    sums[6].third()
    sums[7].third()
    sums[4].last()
    o_small[...] = add.total()
    for n in range(5, 8):
        sums[n].last()

    add.finish()
    for group in groups + sums:
        group.finish()
    for copy in pending:
        copy.wait_send()


def shards_fast(
    inputs,
    w_qkv,
    qv_bias,
    w_out,
    out_bias,
    norm1_gain,
    norm1_shift,
    w_in,
    ffn_bias,
    w_down,
    down_bias,
    norm2_gain,
    norm2_shift,
    attn_drop,
    ffn_drop,
    lengths,
    cotangent,
    pooled,
    positive,
):
    f32, bf16, i32 = jnp.float32, jnp.bfloat16, jnp.int32
    width, half, cols = 768, 256, 384
    dp, cores = lax.axis_size("dp"), lax.axis_size("tensor")
    tail, wide, thin = (LINE, 4, 48), (48, 768), (48, 384)
    shape = jax.ShapeDtypeStruct
    vmem = pl.BlockSpec(memory_space=pltpu.VMEM)
    hbm = pl.BlockSpec(memory_space=pl.ANY)
    smem = pl.BlockSpec(memory_space=pltpu.SMEM)
    scratch = [
        VMEM((3,) + tail + (cols,), bf16), VMEM(tail + (cols,), bf16),
        VMEM((2,) + tail + (width,), bf16), VMEM((2,) + tail + (width,), bf16),
        VMEM((LINE, 4, 8, width), f32), VMEM((8, width), f32),
        VMEM((2, 2, half, width), bf16), VMEM((3, 2, 2 * half, cols), bf16), VMEM((6, 8, 2 * half), f32),
        VMEM((2, 2 * half, cols), bf16), VMEM((2, half, width), bf16), VMEM((2, half, width), bf16),
        VMEM((2, half, width), f32), VMEM((2, half, width), f32), VMEM((2, half, width), f32), VMEM((2, half, 1), f32),
        VMEM((2, 2, half, width), bf16), VMEM((2, 2, 2, half, width), bf16), VMEM((2, 2, 2, half, width), bf16),
        VMEM((2, half, width), f32), VMEM((2, 2, half, width), bf16), VMEM((2, 2, half, width), bf16),
        VMEM((2, 2 * half, cols), bf16), VMEM((3, 2, 2 * half, cols), bf16),
        VMEM((2, half, width), i32), VMEM((2, half, width), i32), VMEM((2, half, width), bf16),
        VMEM((4, LINE, 4) + wide, bf16), VMEM((4, LINE, 4) + thin, bf16),
        VMEM((4, 2, LINE) + wide, bf16), VMEM((4, 2, LINE) + thin, bf16),
        VMEM((4, LINE) + wide, bf16), VMEM((4, LINE) + thin, bf16),
        VMEM((4, 3) + wide, bf16), VMEM((4, 3) + thin, bf16),
        VMEM((4, 16, width), f32), VMEM((3, 16, width), f32), VMEM((LINE, 16, width), f32),
        DMA((9, 6)), DMA((9, 6)), DMA((9,)), DMA((8, 6)), DMA((8, 6)), DMA((6,)), DMA((6,)), DMA((8, 2)), DMA((8, 2)),
        DMA((4,)),
    ]
    outs = [
        shape((2, half, width), bf16), shape((2, half, width), bf16), shape((3,) + thin, f32), shape(thin, f32),
        shape((48, 1536), f32), shape((48, 1536), f32), shape((16, width), f32),
    ]
    gains = jnp.stack([norm1_gain, norm1_shift, norm2_gain, norm2_shift])
    y, dx, d_qkv, d_out, d_in, d_down, total = pl.pallas_call(
        step_kernel,
        out_shape=outs,
        in_specs=[hbm] * 4 + [vmem] * 10 + [smem] * 2,
        out_specs=[vmem] * 7,
        scratch_shapes=scratch,
        compiler_params=pltpu.CompilerParams(collective_id=0, has_side_effects=True, vmem_limit_bytes=67043328),
        name="encoder_step",
    )(
        inputs[:, 0], attn_drop[:, 0], ffn_drop[:, 0], cotangent[:, 0],
        w_qkv, w_out.T, w_in, w_down.T, qv_bias, out_bias[None], ffn_bias.reshape(2, width), down_bias[None], gains,
        pooled, lengths, positive,
    )
    return (
        y[:, None],
        dx[:, None],
        d_qkv,
        total[8].reshape(2, -1),
        d_out.T,
        total[0],
        total[2],
        total[3],
        d_in,
        total[9:11].reshape(-1),
        d_down.T,
        total[1],
        total[4],
        total[5],
        total[6, 0] / (dp * cores),
    )


def solution(mesh):
    placed = (
        P(None, "dp", "tensor", None),
        P(None, "dp", "tensor"),
        P(None, "tensor"),
        P("tensor", "dp"),
        P(),
        P(),
        P(),
        P("dp", "tensor"),
        P("tensor"),
        P("tensor", "dp"),
        P(),
        P(),
        P(),
        P(None, "dp", "tensor", None),
        P(None, "dp", "tensor", None),
        P("dp"),
        P(None, "dp", "tensor", None),
        P(None, "dp", None),
        P("dp"),
    )
    fits = mesh.shape["dp"] == 4 * LINE and mesh.shape["tensor"] == 2
    return jax.shard_map(
        shards_fast if fits else shards,
        mesh=mesh,
        in_specs=placed,
        out_specs=(
            P(None, "dp", "tensor", None),
            P(None, "dp", "tensor", None),
            P(None, "dp", "tensor"),
            P(None, "tensor"),
            P("tensor", "dp"),
            P(),
            P(),
            P(),
            P("dp", "tensor"),
            P("tensor"),
            P("tensor", "dp"),
            P(),
            P(),
            P(),
            P(),
        ),
        check_vma=False,
    )
```
